32 devices in a mesh: grp: 2 (over y), seq: 16 (over z, x, core), head: 1.
Axes of the slice: x: 2, y: 2, z: 4, core: 2. Of those that a mesh axis runs over, the one named last changes fastest.
Arguments:
- queries: bfloat16 [2048, 1, 128], P(('grp', 'seq'), 'head'), parts along dimension 0, may hold values from -6 to 6
- keys: bfloat16 [256, 512, 8, 128], P(('grp', 'seq'), None, 'head'), parts along dimension 0, may hold values from -28 to 28
- values: bfloat16 [256, 512, 8, 128], P(('grp', 'seq'), None, 'head'), parts along dimension 0, may hold values from -6 to 6
- lengths: int32 [32], P('grp'), parts along dimension 0, may hold values from 1 to 4096, 40960 in all
- slot_block: int32 [256], P(('grp', 'seq')), parts along dimension 0, may hold values from 0 to 127, each once
Outputs:
- attended: bfloat16 [2048, 1, 128], P(('grp', 'seq'), 'head'), parts along dimension 0
The draws below stay inside these ranges and needn't reach their ends.
There are 2 independent parts, one for each index of `grp`. The reference program is written for one: setup_inputs(seed, part) draws one part's arguments, and reference() takes and returns one part's arrays. A program takes and returns all parts, laid end to end along the dimension named above; each array names one. Nothing has to cross between parts.
Inputs may be any that keep to these rules, and one draw needn't show every extreme that they name: `slot_block`: each slot holds a different logical block; every block of every sequence has a slot. `lengths`: every sequence has at least one token.
All inputs are finite; a program needn't handle non-finite values.
Results may differ from the reference program's by a relative error of at most 0.0055.
Values may be sent and summed in bfloat16 or wider, within the bound.
No kernel may reach another device: no remote copies, remote signals or barrier semaphores. Data moves between devices by JAX's collectives and lax.ppermute only.
A program may use at most 64 MiB of HBM per device.

```python
import math
import jax
import jax.numpy as jnp
import numpy as np
from jax import lax

QH = 64
KVH = 8
HD = 128
BLK = 512
BATCH = 16
SLOTS = 128
MAXLEN = 4096
N_HEAD = 1


def draw_queries(key, part):
    base = jnp.clip(jax.random.normal(jax.random.fold_in(key, 21), (BATCH, QH, HD), jnp.float32), -6.0, 6.0)
    base = base.reshape(BATCH, N_HEAD, QH // N_HEAD, HD).transpose(0, 2, 1, 3)
    return base.reshape(BATCH * QH // N_HEAD, N_HEAD, HD).astype(jnp.bfloat16)


def draw_keys(key, part):
    base = jnp.clip(3.0 * jax.random.normal(jax.random.fold_in(key, 31), (SLOTS, BLK, KVH, HD), jnp.float32), -18.0, 18.0)
    return base.astype(jnp.bfloat16)


def steps_of(rng, shape, pieces, low, top_value):
    factor_of = 1.0
    for axis_at, shards_of in pieces:
        draws = jax.random.uniform(jax.random.fold_in(jax.random.fold_in(rng, 6), axis_at), (shards_of,), jnp.float32, low / len(pieces), top_value / len(pieces))
        factor_of = factor_of * jnp.repeat(jnp.exp(draws), shape[axis_at] // shards_of).reshape((-1,) + (1,) * (len(shape) - 1 - axis_at))
    return factor_of


def length_profile(number_of, total, most, lean):
    portions = [(1 << 20) // math.isqrt(rank ** lean) + 1 for rank in range(2, number_of + 1)]
    surplus, counts = total - most - (number_of - 1), [1] * (number_of - 1)
    while surplus > 0:
        candidates = [i for i in range(number_of - 1) if counts[i] < most]
        mass, remaining = sum([portions[i] for i in candidates]), surplus
        for i in candidates:
            more = min(most - counts[i], max(1, remaining * portions[i] // mass), surplus)
            counts[i] = counts[i] + more
            surplus = surplus - more
    return np.array([most] + counts)


def ragged_sizes(key, number_of, total, limit, lean):
    if number_of == 2:
        one = jax.random.randint(key, (), max(1, total - limit), min(limit, total - 1) + 1)
        return jnp.stack([one, total - one])
    sizes = jnp.asarray(length_profile(number_of, total, limit, lean), jnp.int32)
    couples = (number_of - 1) // 2
    giver, taker = sizes[1:1 + 2 * couples:2], sizes[2:2 + 2 * couples:2]
    margin = jnp.minimum(giver - 1, limit - taker)
    passed = jax.random.randint(jax.random.fold_in(key, 1), (couples,), 0, 1 << 20) % (margin + 1)
    sizes = sizes.at[1:1 + 2 * couples:2].set(giver - passed).at[2:2 + 2 * couples:2].set(taker + passed)
    return sizes[jax.random.permutation(jax.random.fold_in(key, 2), number_of)]


def bell_draw(stream_key, extent, width, reach, split=(), held_as=jnp.bfloat16):
    values = jax.random.normal(stream_key, extent, jnp.float32) * width
    if len(split) > 0:
        values = steps_of(stream_key, extent, split, -0.22, 0.18) * values
    return jnp.clip(values, min=-reach, max=reach).astype(held_as)


def setup_inputs(seed: int = 0, part: int = 0) -> dict:
    seeds = jax.random.split(jax.random.key(seed), 6)
    part_splits = jax.random.split(jax.random.fold_in(seeds[5], part), 6)
    queries = draw_queries(jax.random.fold_in(jax.random.fold_in(seeds[5], part), 71), part)
    keys = draw_keys(jax.random.fold_in(jax.random.fold_in(seeds[5], part), 71), part)
    values = bell_draw(part_splits[2], (SLOTS, BLK, KVH, HD), 1.0, 6.0, ((0, 16),))
    lengths = ragged_sizes(part_splits[3], BATCH, 5 * MAXLEN // 8 * BATCH, MAXLEN, 1).astype(jnp.int32)
    slot_block = jax.random.permutation(part_splits[4], SLOTS).astype(jnp.int32)
    return {"queries": queries, "keys": keys, "values": values, "lengths": lengths, "slot_block": slot_block}


def reference(queries, keys, values, lengths, slot_block):
    per_half = QH // N_HEAD
    group = QH // KVH
    per_seq = SLOTS // BATCH
    factor = HD ** -0.5
    q_full = queries.reshape(BATCH, per_half, N_HEAD, HD).transpose(0, 2, 1, 3).reshape(BATCH, KVH, group, HD)

    def one_slot(packed):
        key_blk, val_blk, code = packed
        seq_id = (code // per_seq).astype(jnp.int32)
        blk_id = (code % per_seq).astype(jnp.int32)
        q_one = lax.dynamic_index_in_dim(q_full, seq_id, 0, keepdims=False)
        scores = jnp.einsum('kgd,tkd->kgt', q_one.astype(jnp.float32), key_blk.astype(jnp.float32), precision=lax.Precision.HIGHEST) * factor
        positions = blk_id * BLK + jnp.arange(BLK, dtype=jnp.int32)
        live = (positions < lengths[seq_id])[None, None, :]
        peak = jnp.max(jnp.where(live, scores, -1e30), axis=-1)
        weights = jnp.where(live, jnp.exp(scores - peak[..., None]), 0.0).astype(jnp.bfloat16)
        total = jnp.sum(weights.astype(jnp.float32), axis=-1)
        partial_out = jnp.einsum('kgt,tkd->kgd', weights.astype(jnp.float32), val_blk.astype(jnp.float32), precision=lax.Precision.HIGHEST)
        return peak, total, partial_out

    peaks, totals, partials = lax.map(one_slot, (keys, values, slot_block))
    seq_of = (slot_block // per_seq).astype(jnp.int32)
    member = seq_of[:, None] == jnp.arange(BATCH, dtype=jnp.int32)[None, :]
    best = jnp.max(jnp.where(member[:, :, None, None], peaks[:, None], -1e30), axis=0)
    scaled = jnp.exp(peaks - jnp.take(best, seq_of, axis=0))
    denom = jax.ops.segment_sum(scaled * totals, seq_of, BATCH)
    numer = jax.ops.segment_sum(scaled[..., None] * partials, seq_of, BATCH)
    result = numer / denom[..., None]
    result = result.reshape(BATCH, N_HEAD, per_half, HD).transpose(0, 2, 1, 3).reshape(BATCH * per_half, N_HEAD, HD)
    return result.astype(jnp.bfloat16)
```

```python
import functools

import jax
import jax.numpy as jnp
from jax import lax
from jax.experimental import pallas as pl
from jax.experimental.pallas import tpu as pltpu
from jax.sharding import PartitionSpec as P

NEG = -1e30
LOG2E = 1.4426950408889634
EXTRA = 16


def gather_rows(queries, n):
    rows = queries
    step = 1
    while step < n:
        other = lax.ppermute(rows, "seq", [(i, i ^ step) for i in range(n)])
        rows = jnp.concatenate([rows, other], axis=0)
        step *= 2
    return rows


def attend_kernel(
    code_ref, len_ref, at_ref, q_ref, k_ref, v_ref, out_ref, acc_ref, m_ref, l_ref, *, per_seq, block, kv, factor
):
    step = pl.program_id(0)
    batch, heads, head_dim = acc_ref.shape
    cols = block * kv
    group = heads // kv

    @pl.when(step == 0)
    def _():
        m_ref[...] = jnp.full(m_ref.shape, NEG, jnp.float32)
        l_ref[...] = jnp.zeros(l_ref.shape, jnp.float32)
        acc_ref[...] = jnp.zeros(acc_ref.shape, jnp.float32)

    code = code_ref[step]
    seq = code // per_seq
    live_tokens = len_ref[seq] - (code % per_seq) * block

    @pl.when(live_tokens > 0)
    def _():
        q = q_ref[at_ref[step]]
        s = lax.dot_general(q, k_ref[0], (((1,), (1,)), ((), ())), preferred_element_type=jnp.float32)
        col = lax.broadcasted_iota(jnp.int32, (heads, cols), 1)
        row = lax.broadcasted_iota(jnp.int32, (heads, cols), 0)
        keep = (col % kv == row // group) & (col < live_tokens * kv)
        t = jnp.where(keep, s * (factor * LOG2E), NEG)
        peak = jnp.max(t, axis=1, keepdims=True)
        w = jnp.exp2(t - peak).astype(jnp.bfloat16)
        total = jnp.sum(w.astype(jnp.float32), axis=1, keepdims=True)
        part = jnp.dot(w, v_ref[0], preferred_element_type=jnp.float32)
        m_old = m_ref[seq]
        m_new = jnp.maximum(m_old, peak)
        a = jnp.exp2(m_old - m_new)
        c = jnp.exp2(peak - m_new)
        m_ref[seq] = m_new
        l_ref[seq] = l_ref[seq] * a + total * c
        acc_ref[seq] = acc_ref[seq] * a + part * c

    @pl.when(step == pl.num_programs(0) - 1)
    def _():
        eye = lax.broadcasted_iota(jnp.int32, (heads, heads), 0) == lax.broadcasted_iota(
            jnp.int32, (heads, heads), 1
        )
        line = lax.broadcasted_iota(jnp.int32, (EXTRA, heads), 0)
        for b in range(batch):
            l = l_ref[b]
            some = l > 0.0
            scale = jnp.where(some, 1.0 / jnp.where(some, l, 1.0), 0.0)
            out_ref[b, :heads] = (acc_ref[b] * scale).astype(jnp.bfloat16)
            lse = jnp.where(some, m_ref[b] + jnp.log2(jnp.where(some, l, 1.0)), NEG)
            flat = jnp.sum(jnp.where(eye, lse[:, :heads], 0.0), axis=0, keepdims=True)
            high = flat.astype(jnp.bfloat16).astype(jnp.float32)
            rest = flat - high
            mid = rest.astype(jnp.bfloat16).astype(jnp.float32)
            low = rest - mid
            pack = jnp.where(line == 0, high, jnp.where(line == 1, mid, jnp.where(line == 2, low, 0.0)))
            out_ref[b, heads:, :heads] = pack.astype(jnp.bfloat16)
            if heads < head_dim:
                out_ref[b, heads:, heads:] = jnp.zeros((EXTRA, head_dim - heads), jnp.bfloat16)


def merge_kernel(in_ref, out_ref):
    n, span, head_dim = in_ref.shape
    heads = out_ref.shape[0]
    lses = []
    for i in range(n):
        tail = in_ref[i, heads:].astype(jnp.float32)
        lses.append(tail[0:1] + tail[1:2] + tail[2:3])
    best = functools.reduce(jnp.maximum, lses)
    ws = [jnp.exp2(x - best) for x in lses]
    inv = 1.0 / functools.reduce(jnp.add, ws)
    eye = lax.broadcasted_iota(jnp.int32, (heads, head_dim), 0) == lax.broadcasted_iota(
        jnp.int32, (heads, head_dim), 1
    )
    acc = jnp.zeros((heads, head_dim), jnp.float32)
    for i in range(n):
        w = jnp.sum(jnp.where(eye, ws[i] * inv, 0.0), axis=1, keepdims=True)
        acc = acc + w * in_ref[i, :heads].astype(jnp.float32)
    out_ref[...] = acc.astype(jnp.bfloat16)


def body(queries, keys, values, lengths, slot_block):
    n = lax.axis_size("seq")
    slots, block, kv, head_dim = keys.shape
    batch = lengths.shape[0]
    share = queries.shape[0]
    per_seq = slots * n // batch
    heads = share * n // batch
    me = lax.axis_index("seq")
    seq_of = slot_block // per_seq
    local = queries.reshape(share, head_dim)
    if share == heads and n & (n - 1) == 0:
        rows = gather_rows(local, n)
        at = seq_of ^ me
    else:
        rows = lax.all_gather(local, "seq", axis=0, tiled=True)
        at = seq_of
    cols = block * kv
    kernel = functools.partial(attend_kernel, per_seq=per_seq, block=block, kv=kv, factor=head_dim**-0.5)
    packed = pl.pallas_call(
        kernel,
        grid_spec=pltpu.PrefetchScalarGridSpec(
            num_scalar_prefetch=3,
            grid=(slots,),
            in_specs=[
                pl.BlockSpec((batch, heads, head_dim), lambda s, *_: (0, 0, 0)),
                pl.BlockSpec((1, cols, head_dim), lambda s, *_: (s, 0, 0)),
                pl.BlockSpec((1, cols, head_dim), lambda s, *_: (s, 0, 0)),
            ],
            out_specs=pl.BlockSpec((batch, heads + EXTRA, head_dim), lambda s, *_: (0, 0, 0)),
            scratch_shapes=[
                pltpu.VMEM((batch, heads, head_dim), jnp.float32),
                pltpu.VMEM((batch, heads, head_dim), jnp.float32),
                pltpu.VMEM((batch, heads, head_dim), jnp.float32),
            ],
        ),
        out_shape=jax.ShapeDtypeStruct((batch, heads + EXTRA, head_dim), jnp.bfloat16),
        compiler_params=pltpu.CompilerParams(vmem_limit_bytes=32 * 1024 * 1024),
        name="attend",
    )(
        slot_block,
        lengths,
        at,
        rows.reshape(batch, heads, head_dim),
        keys.reshape(slots, cols, head_dim),
        values.reshape(slots, cols, head_dim),
    )
    if share != heads:
        lse = packed[:, heads:, :heads].transpose(0, 2, 1).reshape(n, share, EXTRA)
        tail = jnp.zeros((n, EXTRA, head_dim), jnp.bfloat16).at[:, :, :share].set(lse.transpose(0, 2, 1))
        packed = jnp.concatenate([packed[:, :heads].reshape(n, share, head_dim), tail], axis=1)
    got = lax.all_to_all(packed, "seq", 0, 0, tiled=True)
    result = pl.pallas_call(
        merge_kernel,
        out_shape=jax.ShapeDtypeStruct((share, head_dim), jnp.bfloat16),
        compiler_params=pltpu.CompilerParams(vmem_limit_bytes=16 * 1024 * 1024),
        name="merge",
    )(got)
    return result.reshape(share, 1, head_dim)


def solution(mesh):
    placed = (
        P(("grp", "seq"), "head", None),
        P(("grp", "seq"), None, "head", None),
        P(("grp", "seq"), None, "head", None),
        P("grp"),
        P(("grp", "seq")),
    )
    return jax.shard_map(
        body, mesh=mesh, in_specs=placed, out_specs=P(("grp", "seq"), "head", None), check_vma=False
    )
```

```python
import functools

import jax
import jax.numpy as jnp
from jax import lax
from jax.experimental import pallas as pl
from jax.experimental.pallas import tpu as pltpu
from jax.sharding import PartitionSpec as P


NEG = -1e30
LOG2E = 1.4426950408889634
EXTRA = 8
CHUNK = 1024
SPREAD_FLOPS = 1_000_000_000
PIECES = 2


def join_kernel(a_ref, b_ref, out_ref):
    size = a_ref.shape[0]
    out_ref[:size] = a_ref[...]
    out_ref[size:] = b_ref[...]


def join(a, b):
    return pl.pallas_call(
        join_kernel,
        out_shape=jax.ShapeDtypeStruct((2 * a.shape[0], a.shape[1]), a.dtype),
        compiler_params=pltpu.CompilerParams(vmem_limit_bytes=4 * 1024 * 1024),
        name="join",
    )(a, b)


def steps_of(n):
    return [n >> (i + 1) for i in range(n.bit_length() - 1)]


def gather_rows(queries, n):
    rows = queries
    steps = steps_of(n)
    for hop, step in enumerate(steps):
        other = lax.ppermute(rows, "seq", [(i, i ^ step) for i in range(n)])
        if hop + 1 < len(steps):
            rows = join(rows, other)
    return rows, other


def spread_kernel(src_ref, out_ref, sem):
    copies = [
        pltpu.make_async_copy(src_ref.at[:, :, p], out_ref.at[:, p], sem.at[p]) for p in range(src_ref.shape[2])
    ]
    for copy in copies:
        copy.start()
    for copy in copies:
        copy.wait()


def spread(view, first, count):
    slots, block, parts, width, head_dim = view.shape

    def kernel(src_ref, out_ref, sem):
        spread_kernel(src_ref.at[pl.ds(first, count)], out_ref, sem)

    out = pl.pallas_call(
        kernel,
        in_specs=[pl.BlockSpec(memory_space=pltpu.HBM)],
        out_specs=pl.BlockSpec(memory_space=pltpu.VMEM),
        out_shape=pltpu.VMEM((count, parts, block, width, head_dim), view.dtype),
        scratch_shapes=[pltpu.SemaphoreType.DMA((parts,))],
        compiler_params=pltpu.CompilerParams(vmem_limit_bytes=8 * 1024 * 1024),
        cost_estimate=pl.CostEstimate(flops=SPREAD_FLOPS, transcendentals=0, bytes_accessed=view.nbytes * count // slots),
        name="spread",
    )(view)
    return out.reshape(count, parts, block * width, head_dim)


def attend_kernel(code_ref, len_ref, near_ref, far_ref, *rest, place, per_seq, block, kv, parts, factor):
    pieces = (len(rest) - 5) // 2
    k_refs, v_refs = rest[:pieces], rest[pieces : 2 * pieces]
    out_ref, acc_ref, m_ref, l_ref, s_ref = rest[2 * pieces :]
    batch, heads, head_dim = acc_ref.shape
    each, _, cols, _ = k_refs[0].shape
    slots = each * pieces
    group = heads // kv
    width = kv // parts
    span = heads // parts
    chunk = min(CHUNK, cols)
    tile = 128
    lane = lax.broadcasted_iota(jnp.int32, (heads, tile), 1)
    row = lax.broadcasted_iota(jnp.int32, (heads, tile), 0)
    match = jnp.where(lane % width == (row // group) % width, 0.0, NEG)
    eye = lax.broadcasted_iota(jnp.int32, (heads, heads), 0) == lax.broadcasted_iota(jnp.int32, (heads, heads), 1)
    line = lax.broadcasted_iota(jnp.int32, (EXTRA, head_dim), 0)
    m_ref[...] = jnp.full(m_ref.shape, NEG, jnp.float32)
    l_ref[...] = jnp.zeros(l_ref.shape, jnp.float32)
    acc_ref[...] = jnp.zeros(acc_ref.shape, jnp.float32)
    empty = jnp.where(line == 0, NEG, 0.0).astype(jnp.bfloat16)
    for b in range(batch):
        out_ref[b, :heads] = jnp.zeros((heads, head_dim), jnp.bfloat16)
        out_ref[b, heads:] = empty

    starts = range(0, cols, chunk)
    scale2 = factor * LOG2E

    def setup(slot):
        code = code_ref[slot]
        seq = code // per_seq
        limit = (len_ref[seq] - (code % per_seq) * block) * width
        half, at = place(seq)
        return {"seq": seq, "limit": limit, "q": jnp.where(half == 0, near_ref[at], far_ref[at]), "top": None}

    def score(slot, state, start):
        s = jnp.concatenate(
            [
                lax.dot_general(
                    state["q"][p * span : (p + 1) * span],
                    k_refs[slot // each][slot % each, p, pl.ds(start, chunk)],
                    (((1,), (1,)), ((), ())),
                    preferred_element_type=jnp.float32,
                )
                for p in range(parts)
            ],
            axis=0,
        )
        top = state["top"]
        for j in range(0, chunk, tile):
            t = s[:, j : j + tile] + jnp.where(lane < state["limit"] - (start + j), 0.0, NEG)
            s_ref[slot % 2, :, pl.ds(start + j, tile)] = t
            top = t if top is None else jnp.maximum(top, t)
        state["top"] = top

    def peak_of(state):
        top = jnp.max(state["top"] + match, axis=1, keepdims=True)
        state["peak"] = jnp.maximum(top, 0.5 * NEG) * scale2
        state["shift"] = match - state["peak"]
        state["part"] = jnp.zeros((heads, head_dim), jnp.float32)
        state["total"] = jnp.zeros((heads, tile), jnp.float32)

    def weigh(slot, state, start):
        ws = []
        for j in range(0, chunk, tile):
            w = jnp.exp2(s_ref[slot % 2, :, pl.ds(start + j, tile)] * scale2 + state["shift"])
            state["total"] = state["total"] + w
            ws.append(w.astype(jnp.bfloat16))
        w = jnp.concatenate(ws, axis=1)
        state["part"] = state["part"] + jnp.concatenate(
            [
                jnp.dot(
                    w[p * span : (p + 1) * span],
                    v_refs[slot // each][slot % each, p, pl.ds(start, chunk)],
                    preferred_element_type=jnp.float32,
                )
                for p in range(parts)
            ],
            axis=0,
        )

    def fold(state):
        seq, peak, part = state["seq"], state["peak"], state["part"]
        total = jnp.sum(state["total"], axis=1, keepdims=True)
        m_old = m_ref[seq]
        m_new = jnp.maximum(m_old, peak)
        a = jnp.exp2(m_old - m_new)
        c = jnp.exp2(peak - m_new)
        m_ref[seq] = m_new
        l_ref[seq] = l_ref[seq] * a + total * c
        acc_ref[seq] = acc_ref[seq] * a + part * c

    now = setup(0)
    for start in starts:
        score(0, now, start)
    peak_of(now)
    for slot in range(slots):
        ahead = setup(slot + 1) if slot + 1 < slots else None
        for start in starts:
            if ahead is not None:
                score(slot + 1, ahead, start)
            weigh(slot, now, start)
        fold(now)
        if ahead is not None:
            peak_of(ahead)
        now = ahead

    for slot in range(slots):
        seq = code_ref[slot] // per_seq
        l = l_ref[seq]
        some = l > 0.0
        scale = jnp.where(some, 1.0 / jnp.where(some, l, 1.0), 0.0)
        out_ref[seq, :heads] = (acc_ref[seq] * scale).astype(jnp.bfloat16)
        lse = jnp.where(some, m_ref[seq] + jnp.log2(jnp.where(some, l, 1.0)), NEG)
        flat = jnp.sum(jnp.where(eye, lse[:, :heads], 0.0), axis=0, keepdims=True)
        high = flat.astype(jnp.bfloat16).astype(jnp.float32)
        rest = flat - high
        mid = rest.astype(jnp.bfloat16).astype(jnp.float32)
        low = rest - mid
        place_in = line[:, :heads]
        pack = jnp.where(place_in == 0, high, jnp.where(place_in == 1, mid, jnp.where(place_in == 2, low, 0.0)))
        out_ref[seq, heads:, :heads] = pack.astype(jnp.bfloat16)


def merge_kernel(in_ref, out_ref):
    n, _, head_dim = in_ref.shape
    heads = out_ref.shape[0]
    lses = []
    for i in range(n):
        tail = in_ref[i, heads:].astype(jnp.float32)
        lses.append(tail[0:1] + tail[1:2] + tail[2:3])
    best = functools.reduce(jnp.maximum, lses)
    ws = [jnp.exp2(x - best) for x in lses]
    inv = 1.0 / functools.reduce(jnp.add, ws)
    eye = lax.broadcasted_iota(jnp.int32, (heads, head_dim), 0) == lax.broadcasted_iota(
        jnp.int32, (heads, head_dim), 1
    )
    acc = jnp.zeros((heads, head_dim), jnp.float32)
    for i in range(n):
        w = jnp.sum(jnp.where(eye, ws[i] * inv, 0.0), axis=1, keepdims=True)
        acc = acc + w * in_ref[i, :heads].astype(jnp.float32)
    out_ref[...] = acc.astype(jnp.bfloat16)


def body(queries, keys, values, lengths, slot_block):
    n = lax.axis_size("seq")
    slots, block, kv, head_dim = keys.shape
    batch = lengths.shape[0]
    share = queries.shape[0]
    per_seq = slots * n // batch
    heads = share * n // batch
    local = queries.reshape(share, head_dim)
    if share == heads and n & (n - 1) == 0 and n > 1:
        near, far = gather_rows(local, n)
        steps = steps_of(n)

        def place(seq):
            away = seq ^ lax.axis_index("seq")
            at = jnp.int32(0)
            for i, step in enumerate(steps[:-1]):
                at = at | jnp.where((away & step) != 0, 1 << i, 0)
            return away & steps[-1], at

    else:
        near = far = lax.all_gather(local, "seq", axis=0, tiled=True)

        def place(seq):
            return jnp.int32(0), seq

    near = near.reshape(-1, heads, head_dim)
    far = far.reshape(-1, heads, head_dim)
    parts = kv // 2 if kv % 2 == 0 else 1
    width = kv // parts
    cols = block * width

    pieces = PIECES if slots % PIECES == 0 else 1

    def split(cache):
        view = pltpu.with_memory_space_constraint(cache.reshape(slots, block, parts, width, head_dim), pltpu.HBM)
        out = []
        for i in range(pieces):
            out.append(spread(view, i * (slots // pieces), slots // pieces))
        return out

    kernel = functools.partial(
        attend_kernel, place=place, per_seq=per_seq, block=block, kv=kv, parts=parts, factor=head_dim**-0.5
    )
    packed = pl.pallas_call(
        kernel,
        in_specs=[
            pl.BlockSpec(memory_space=pltpu.SMEM),
            pl.BlockSpec(memory_space=pltpu.SMEM),
            *[pl.BlockSpec(memory_space=pltpu.VMEM)] * (2 + 2 * pieces),
        ],
        out_specs=pl.BlockSpec(memory_space=pltpu.VMEM),
        scratch_shapes=[
            pltpu.VMEM((batch, heads, head_dim), jnp.float32),
            pltpu.VMEM((batch, heads, head_dim), jnp.float32),
            pltpu.VMEM((batch, heads, head_dim), jnp.float32),
            pltpu.VMEM((2, heads, cols), jnp.float32),
        ],
        out_shape=jax.ShapeDtypeStruct((batch, heads + EXTRA, head_dim), jnp.bfloat16),
        compiler_params=pltpu.CompilerParams(vmem_limit_bytes=32 * 1024 * 1024),
        name="attend",
    )(slot_block, lengths, near, far, *split(keys), *split(values))
    if share != heads:
        lse = packed[:, heads:, :heads].transpose(0, 2, 1).reshape(n, share, EXTRA)
        tail = jnp.zeros((n, EXTRA, head_dim), jnp.bfloat16).at[:, :, :share].set(lse.transpose(0, 2, 1))
        packed = jnp.concatenate([packed[:, :heads].reshape(n, share, head_dim), tail], axis=1)
    got = lax.all_to_all(packed, "seq", 0, 0, tiled=True)
    result = pl.pallas_call(
        merge_kernel,
        out_shape=jax.ShapeDtypeStruct((share, head_dim), jnp.bfloat16),
        compiler_params=pltpu.CompilerParams(vmem_limit_bytes=16 * 1024 * 1024),
        name="merge",
    )(got)
    return result.reshape(share, 1, head_dim)


def solution(mesh):
    placed = (
        P(("grp", "seq"), "head", None),
        P(("grp", "seq"), None, "head", None),
        P(("grp", "seq"), None, "head", None),
        P("grp"),
        P(("grp", "seq")),
    )
    return jax.shard_map(
        body, mesh=mesh, in_specs=placed, out_specs=P(("grp", "seq"), "head", None), check_vma=False
    )
```

```python
import functools

import jax
import jax.numpy as jnp
from jax import lax
from jax.experimental import pallas as pl
from jax.experimental.pallas import tpu as pltpu
from jax.sharding import PartitionSpec as P


NEG = -1e30
LOG2E = 1.4426950408889634
TILE = 128
EXTRA = 8
CHUNK = 1024
MIB = 1024 * 1024
SPREAD_FLOPS = 1_000_000_000
VMEM = pl.BlockSpec(memory_space=pltpu.VMEM)
SMEM = pl.BlockSpec(memory_space=pltpu.SMEM)
HBM = pl.BlockSpec(memory_space=pltpu.HBM)


def limit(mib):
    return pltpu.CompilerParams(vmem_limit_bytes=mib * MIB)


def join_kernel(*refs):
    out_ref = refs[-1]
    size = refs[0].shape[0]
    for i, ref in enumerate(refs[:-1]):
        out_ref[i * size : (i + 1) * size] = ref[...]


def join(*rows):
    return pl.pallas_call(
        join_kernel,
        out_shape=jax.ShapeDtypeStruct((len(rows) * rows[0].shape[0], rows[0].shape[1]), rows[0].dtype),
        compiler_params=limit(4),
        name="join",
    )(*rows)


def steps_of(n):
    return [n >> (i + 1) for i in range(n.bit_length() - 2)]


def gather_rows(queries, n):
    steps = steps_of(n)
    cross = lax.ppermute(queries, "seq", [(i, i ^ steps[0] ^ 1) for i in range(n)])
    up = lax.ppermute(queries, "seq", [(i, i ^ 1) for i in range(n)])
    rows = queries
    for hop, step in enumerate(steps):
        other = lax.ppermute(rows, "seq", [(i, i ^ step) for i in range(n)])
        rows = join(rows, up, other, cross) if hop == 0 else join(rows, other)
    return rows, rows


def spread_copies(src_ref, out_ref, sem, first, count):
    return [
        pltpu.make_async_copy(src_ref.at[pl.ds(first, count), :, p], out_ref.at[:, p], sem.at[p])
        for p in range(src_ref.shape[2])
    ]


def spread_type(view, count):
    _, block, parts, width, head_dim = view.shape
    return pltpu.VMEM((count, parts, block, width, head_dim), view.dtype)


def by_part(spread_out):
    count, parts, block, width, head_dim = spread_out.shape
    return spread_out.reshape(count, parts, block * width, head_dim)


def spread(view, first, count):
    def kernel(src_ref, out_ref, sem):
        copies = spread_copies(src_ref, out_ref, sem, first, count)
        for copy in copies:
            copy.start()
        for copy in copies:
            copy.wait()

    out = pl.pallas_call(
        kernel,
        in_specs=[HBM],
        out_specs=VMEM,
        out_shape=spread_type(view, count),
        scratch_shapes=[pltpu.SemaphoreType.DMA((view.shape[2],))],
        compiler_params=limit(12),
        cost_estimate=pl.CostEstimate(
            flops=SPREAD_FLOPS, transcendentals=0, bytes_accessed=view.nbytes * count // view.shape[0]
        ),
        name="spread",
    )(view)
    return by_part(out)


def attend_slots(refs, s_ref, sizes, emit):
    code_ref, len_ref, near_ref, far_ref, k_refs, v_refs = refs
    slots = sum(ref.shape[0] for ref in k_refs)
    _, parts, cols, head_dim = k_refs[0].shape
    heads = near_ref.shape[1]
    width = sizes["kv"] // parts
    group = heads // sizes["kv"]
    span = heads // parts
    chunk = min(CHUNK, cols)
    scale2 = head_dim**-0.5 * LOG2E
    lane = lax.broadcasted_iota(jnp.int32, (heads, TILE), 1)
    row = lax.broadcasted_iota(jnp.int32, (heads, TILE), 0)
    match = jnp.where(lane % width == (row // group) % width, 0.0, NEG)
    starts = range(0, cols, chunk)

    def setup(slot):
        code = code_ref[slot]
        seq = code // sizes["per_seq"]
        stop = (len_ref[seq] - (code % sizes["per_seq"]) * (cols // width)) * width
        half, at = sizes["place"](seq)
        return {"seq": seq, "stop": stop, "q": jnp.where(half == 0, near_ref[at], far_ref[at]), "top": None}

    def score(slot, state, start):
        s = jnp.concatenate(
            [
                lax.dot_general(
                    state["q"][p * span : (p + 1) * span],
                    k_refs[slot * len(k_refs) // slots][slot % (slots // len(k_refs)), p, pl.ds(start, chunk)],
                    (((1,), (1,)), ((), ())),
                    preferred_element_type=jnp.float32,
                )
                for p in range(parts)
            ],
            axis=0,
        )
        top = state["top"]
        for j in range(0, chunk, TILE):
            t = s[:, j : j + TILE] + jnp.where(lane < state["stop"] - (start + j), 0.0, NEG)
            s_ref[slot % 2, :, pl.ds(start + j, TILE)] = t
            top = t if top is None else jnp.maximum(top, t)
        state["top"] = top

    def peak_of(state):
        top = jnp.max(state["top"] + match, axis=1, keepdims=True)
        state["peak"] = jnp.maximum(top, 0.5 * NEG) * scale2
        state["shift"] = match - state["peak"]
        state["part"] = jnp.zeros((heads, head_dim), jnp.float32)
        state["total"] = jnp.zeros((heads, TILE), jnp.float32)

    def weigh(slot, state, start):
        ws = []
        for j in range(0, chunk, TILE):
            w = jnp.exp2(s_ref[slot % 2, :, pl.ds(start + j, TILE)] * scale2 + state["shift"])
            state["total"] = state["total"] + w
            ws.append(w.astype(jnp.bfloat16))
        w = jnp.concatenate(ws, axis=1)
        state["part"] = state["part"] + jnp.concatenate(
            [
                jnp.dot(
                    w[p * span : (p + 1) * span],
                    v_refs[slot * len(v_refs) // slots][slot % (slots // len(v_refs)), p, pl.ds(start, chunk)],
                    preferred_element_type=jnp.float32,
                )
                for p in range(parts)
            ],
            axis=0,
        )

    now = setup(0)
    for start in starts:
        score(0, now, start)
    peak_of(now)
    for slot in range(slots):
        ahead = setup(slot + 1) if slot + 1 < slots else None
        for start in starts:
            if ahead is not None:
                score(slot + 1, ahead, start)
            weigh(slot, now, start)
        emit(slot, now["seq"], now["peak"], jnp.sum(now["total"], axis=1, keepdims=True), now["part"])
        if ahead is not None:
            peak_of(ahead)
        now = ahead


def attend_kernel(code_ref, len_ref, near_ref, far_ref, *rest, sizes, pieces, halves):
    k_refs, v_refs, rest = rest[: pieces[0]], rest[pieces[0] : sum(pieces)], rest[sum(pieces) :]
    out_refs = rest[:halves]
    acc_ref, m_ref, l_ref, s_ref = rest[halves:]
    batch, heads, head_dim = acc_ref.shape
    count = batch // halves
    m_ref[...] = jnp.full(m_ref.shape, NEG, jnp.float32)
    l_ref[...] = jnp.zeros(l_ref.shape, jnp.float32)
    acc_ref[...] = jnp.zeros(acc_ref.shape, jnp.float32)

    def fold(slot, seq, peak, total, part):
        at = seq
        if halves == 2:
            at = ((seq & 1) ^ (lax.axis_index("seq") & 1)) * count + (seq >> 1)
        m_old = m_ref[at]
        m_new = jnp.maximum(m_old, peak)
        a = jnp.exp2(m_old - m_new)
        c = jnp.exp2(peak - m_new)
        m_ref[at] = m_new
        l_ref[at] = l_ref[at] * a + total * c
        acc_ref[at] = acc_ref[at] * a + part * c

    attend_slots((code_ref, len_ref, near_ref, far_ref, k_refs, v_refs), s_ref, sizes, fold)
    lane = lax.broadcasted_iota(jnp.int32, (heads, TILE), 1)
    stats = jnp.zeros((heads, TILE), jnp.float32)
    for half in range(halves):
        for i in range(count):
            at = half * count + i
            stats = jnp.where(lane == 2 * half * count + i, m_ref[at], stats)
            stats = jnp.where(lane == (2 * half + 1) * count + i, l_ref[at], stats)
            out_refs[half][i * heads : (i + 1) * heads] = acc_ref[at]
    turned = jnp.transpose(stats, (1, 0))
    for half in range(halves):
        out_refs[half][count * heads :, :heads] = turned[2 * half * count : 2 * (half + 1) * count]
        if heads < head_dim:
            out_refs[half][count * heads :, heads:] = jnp.zeros((2 * count, head_dim - heads), jnp.float32)


def split3(x):
    high = x.astype(jnp.bfloat16).astype(jnp.float32)
    mid = (x - high).astype(jnp.bfloat16).astype(jnp.float32)
    return high, mid, x - high - mid


def pair_kernel(mine_ref, other_ref, out_ref):
    count, rows, head_dim = out_ref.shape
    heads = rows - EXTRA
    base = count * heads
    m1, l1 = mine_ref[base : base + count], mine_ref[base + count :]
    m2, l2 = other_ref[base : base + count], other_ref[base + count :]
    m = jnp.maximum(m1, m2)
    a = jnp.exp2(m1 - m)
    b = jnp.exp2(m2 - m)
    l = a * l1 + b * l2
    some = l > 0.0
    safe = jnp.where(some, l, 1.0)
    inv = jnp.where(some, 1.0 / safe, 0.0)
    lse = jnp.where(some, m + jnp.log2(safe), NEG)
    high, mid, low = split3(lse)
    cols = jnp.transpose(jnp.concatenate([a * inv, b * inv], axis=0), (1, 0))
    line = lax.broadcasted_iota(jnp.int32, (EXTRA, head_dim), 0)
    for i in range(count):
        x = cols[:heads, i : i + 1] * mine_ref[i * heads : (i + 1) * heads]
        y = cols[:heads, count + i : count + i + 1] * other_ref[i * heads : (i + 1) * heads]
        out_ref[i, :heads] = (x + y).astype(jnp.bfloat16)
        pack = jnp.where(line == 0, high[i : i + 1], jnp.where(line == 1, mid[i : i + 1], 0.0))
        out_ref[i, heads:] = jnp.where(line == 2, low[i : i + 1], pack).astype(jnp.bfloat16)


def merge_kernel(in_ref, out_ref):
    n, _, head_dim = in_ref.shape
    heads = out_ref.shape[0]
    lses = []
    for i in range(n):
        tail = in_ref[i, heads:].astype(jnp.float32)
        lses.append(tail[0:1] + tail[1:2] + tail[2:3])
    best = functools.reduce(jnp.maximum, lses)
    ws = [jnp.exp2(x - best) for x in lses]
    inv = 1.0 / functools.reduce(jnp.add, ws)
    eye = lax.broadcasted_iota(jnp.int32, (heads, head_dim), 0) == lax.broadcasted_iota(
        jnp.int32, (heads, head_dim), 1
    )
    acc = jnp.zeros((heads, head_dim), jnp.float32)
    for i in range(n):
        w = jnp.sum(jnp.where(eye, ws[i] * inv, 0.0), axis=1, keepdims=True)
        acc = acc + w * in_ref[i, :heads].astype(jnp.float32)
    out_ref[...] = acc.astype(jnp.bfloat16)


def pack_rows(whole, batch, heads, n, share):
    head_dim = whole.shape[1]
    sums = whole[: batch * heads].reshape(batch, heads, head_dim)
    m = whole[batch * heads : batch * (heads + 1), :heads]
    l = whole[batch * (heads + 1) :, :heads]
    some = l > 0.0
    safe = jnp.where(some, l, 1.0)
    out = jnp.where(some, 1.0 / safe, 0.0)[..., None] * sums
    lse = jnp.where(some, m + jnp.log2(safe), NEG)
    high = lax.reduce_precision(lse, 8, 7)
    mid = lax.reduce_precision(lse - high, 8, 7)
    lines = jnp.stack([x.reshape(n, share) for x in (high, mid, lse - high - mid)], axis=1)
    tail = jnp.zeros((n, EXTRA, head_dim), jnp.float32).at[:, :3, :share].set(lines)
    return jnp.concatenate([out.reshape(n, share, head_dim), tail], axis=1).astype(jnp.bfloat16)


def body(queries, keys, values, lengths, slot_block):
    n = lax.axis_size("seq")
    slots, block, kv, head_dim = keys.shape
    batch = lengths.shape[0]
    share = queries.shape[0]
    heads = share * n // batch
    local = queries.reshape(share, head_dim)
    paired = share == heads and n & (n - 1) == 0 and n > 2
    halves = 2 if paired else 1
    if paired:
        near, far = gather_rows(local, n)
        steps = steps_of(n)

        def place(seq):
            away = seq ^ lax.axis_index("seq")
            at = away & 1
            for i, step in enumerate(steps):
                at = at | jnp.where((away & step) != 0, 2 << i, 0)
            return jnp.int32(0), at

    else:
        near = far = lax.all_gather(local, "seq", axis=0, tiled=True)

        def place(seq):
            return jnp.int32(0), seq

    near = near.reshape(-1, heads, head_dim)
    far = far.reshape(-1, heads, head_dim)
    parts = kv // 2 if kv % 2 == 0 else 1
    sizes = {"kv": kv, "per_seq": slots * n // batch, "place": place}

    def view_of(cache):
        return pltpu.with_memory_space_constraint(cache.reshape(slots, block, parts, kv // parts, head_dim), pltpu.HBM)

    key_view, value_view = view_of(keys), view_of(values)
    pieces = (2 if slots % 2 == 0 else 1, 1)
    blocks = []
    for view, count in zip((key_view, value_view), pieces):
        for i in range(count):
            blocks.append(spread(view, i * (slots // count), slots // count))
    sums = pl.pallas_call(
        functools.partial(attend_kernel, sizes=sizes, pieces=pieces, halves=halves),
        in_specs=[SMEM, SMEM] + [VMEM] * (2 + len(blocks)),
        out_specs=[VMEM] * halves,
        out_shape=[pltpu.VMEM((batch // halves * (heads + 2), head_dim), jnp.float32)] * halves,
        scratch_shapes=[pltpu.VMEM((batch, heads, head_dim), jnp.float32)] * 3
        + [pltpu.VMEM((2, heads, block * kv // parts), jnp.float32)],
        compiler_params=limit(24),
        name="attend",
    )(slot_block, lengths, near, far, *blocks)
    if paired:
        other = lax.ppermute(sums[1], "seq", [(i, i ^ 1) for i in range(n)])
        packed = pl.pallas_call(
            pair_kernel,
            out_shape=jax.ShapeDtypeStruct((batch // 2, heads + EXTRA, head_dim), jnp.bfloat16),
            compiler_params=limit(8),
            name="pair",
        )(sums[0], other)
        groups = [list(range(core, n, 2)) for core in range(2)]
    else:
        packed = pack_rows(sums[0], batch, heads, n, share)
        groups = None
    got = lax.all_to_all(packed, "seq", 0, 0, tiled=True, axis_index_groups=groups)
    result = pl.pallas_call(
        merge_kernel,
        out_shape=jax.ShapeDtypeStruct((share, head_dim), jnp.bfloat16),
        compiler_params=limit(8),
        name="merge",
    )(got)
    return result.reshape(share, 1, head_dim)


def solution(mesh):
    placed = (
        P(("grp", "seq"), "head", None),
        P(("grp", "seq"), None, "head", None),
        P(("grp", "seq"), None, "head", None),
        P("grp"),
        P(("grp", "seq")),
    )
    return jax.shard_map(
        body, mesh=mesh, in_specs=placed, out_specs=P(("grp", "seq"), "head", None), check_vma=False
    )
```

```python
import functools

import jax
import jax.numpy as jnp
from jax import lax
from jax.experimental import pallas as pl
from jax.experimental.pallas import tpu as pltpu
from jax.sharding import PartitionSpec as P


NEG = -1e30
LOG2E = 1.4426950408889634
TILE = 128
EXTRA = 8
CHUNK = 1024
MIB = 1024 * 1024
SPREAD_FLOPS = 1_000_000_000
VMEM = pl.BlockSpec(memory_space=pltpu.VMEM)
SMEM = pl.BlockSpec(memory_space=pltpu.SMEM)
HBM = pl.BlockSpec(memory_space=pltpu.HBM)


def limit(mib):
    return pltpu.CompilerParams(vmem_limit_bytes=mib * MIB)


def join_kernel(*refs):
    out_ref = refs[-1]
    size = refs[0].shape[0]
    for i, ref in enumerate(refs[:-1]):
        out_ref[i * size : (i + 1) * size] = ref[...]


def join(*rows):
    return pl.pallas_call(
        join_kernel,
        out_shape=jax.ShapeDtypeStruct((len(rows) * rows[0].shape[0], rows[0].shape[1]), rows[0].dtype),
        compiler_params=limit(4),
        name="join",
    )(*rows)


def steps_of(n):
    return [n >> (i + 1) for i in range(n.bit_length() - 2)]


def gather_rows(queries, n):
    rows = queries
    steps = steps_of(n)
    for step in steps:
        other = lax.ppermute(rows, "seq", [(i, i ^ step ^ 1) for i in range(n)])
        rows = join(rows, other)
    last = []
    for near in (1,):
        last.append(lax.ppermute(rows, "seq", [(i, i ^ near) for i in range(n)]))
    return [rows, *last]


def spread_copies(src_ref, out_ref, sem, first, count):
    return [
        pltpu.make_async_copy(src_ref.at[pl.ds(first, count), :, p], out_ref.at[:, p], sem.at[p])
        for p in range(src_ref.shape[2])
    ]


def spread_type(view, count):
    _, block, parts, width, head_dim = view.shape
    return pltpu.VMEM((count, parts, block, width, head_dim), view.dtype)


def by_part(spread_out):
    count, parts, block, width, head_dim = spread_out.shape
    return spread_out.reshape(count, parts, block * width, head_dim)


def spread(view, first, count):
    def kernel(src_ref, out_ref, sem):
        copies = spread_copies(src_ref, out_ref, sem, first, count)
        for copy in copies:
            copy.start()
        for copy in copies:
            copy.wait()

    out = pl.pallas_call(
        kernel,
        in_specs=[HBM],
        out_specs=VMEM,
        out_shape=spread_type(view, count),
        scratch_shapes=[pltpu.SemaphoreType.DMA((view.shape[2],))],
        compiler_params=limit(12),
        cost_estimate=pl.CostEstimate(
            flops=SPREAD_FLOPS, transcendentals=0, bytes_accessed=view.nbytes * count // view.shape[0]
        ),
        name="spread",
    )(view)
    return by_part(out)


def attend_slots(refs, s_ref, sizes, emit):
    code_ref, len_ref, row_refs, k_refs, v_refs = refs
    slots = sum(ref.shape[0] for ref in k_refs)
    _, parts, cols, head_dim = k_refs[0].shape
    heads = row_refs[0].shape[1]
    width = sizes["kv"] // parts
    group = heads // sizes["kv"]
    span = heads // parts
    chunk = min(CHUNK, cols)
    scale2 = head_dim**-0.5 * LOG2E
    lane = lax.broadcasted_iota(jnp.int32, (heads, TILE), 1)
    row = lax.broadcasted_iota(jnp.int32, (heads, TILE), 0)
    match = jnp.where(lane % width == (row // group) % width, 0.0, NEG)
    starts = range(0, cols, chunk)

    def setup(slot):
        code = code_ref[slot]
        seq = code // sizes["per_seq"]
        stop = (len_ref[seq] - (code % sizes["per_seq"]) * (cols // width)) * width
        which, at = sizes["place"](seq)
        q = row_refs[0][at]
        for i, ref in enumerate(row_refs[1:]):
            q = jnp.where(which == i + 1, ref[at], q)
        return {"seq": seq, "stop": stop, "q": q, "top": None}

    def score(slot, state, start):
        s = jnp.concatenate(
            [
                lax.dot_general(
                    state["q"][p * span : (p + 1) * span],
                    k_refs[slot * len(k_refs) // slots][slot % (slots // len(k_refs)), p, pl.ds(start, chunk)],
                    (((1,), (1,)), ((), ())),
                    preferred_element_type=jnp.float32,
                )
                for p in range(parts)
            ],
            axis=0,
        )
        top = state["top"]
        for j in range(0, chunk, TILE):
            t = s[:, j : j + TILE] + jnp.where(lane < state["stop"] - (start + j), 0.0, NEG)
            s_ref[slot % 2, :, pl.ds(start + j, TILE)] = t
            top = t if top is None else jnp.maximum(top, t)
        state["top"] = top

    def peak_of(state):
        top = jnp.max(state["top"] + match, axis=1, keepdims=True)
        state["peak"] = jnp.maximum(top, 0.5 * NEG) * scale2
        state["shift"] = match - state["peak"]
        state["part"] = jnp.zeros((heads, head_dim), jnp.float32)
        state["total"] = jnp.zeros((heads, TILE), jnp.float32)

    def weigh(slot, state, start):
        ws = []
        for j in range(0, chunk, TILE):
            w = jnp.exp2(s_ref[slot % 2, :, pl.ds(start + j, TILE)] * scale2 + state["shift"])
            state["total"] = state["total"] + w
            ws.append(w.astype(jnp.bfloat16))
        w = jnp.concatenate(ws, axis=1)
        state["part"] = state["part"] + jnp.concatenate(
            [
                jnp.dot(
                    w[p * span : (p + 1) * span],
                    v_refs[slot * len(v_refs) // slots][slot % (slots // len(v_refs)), p, pl.ds(start, chunk)],
                    preferred_element_type=jnp.float32,
                )
                for p in range(parts)
            ],
            axis=0,
        )

    now = setup(0)
    for start in starts:
        score(0, now, start)
    peak_of(now)
    for slot in range(slots):
        ahead = setup(slot + 1) if slot + 1 < slots else None
        for start in starts:
            if ahead is not None:
                score(slot + 1, ahead, start)
            weigh(slot, now, start)
        if ahead is not None:
            peak_of(ahead)
        emit(slot, now["seq"], now["peak"], jnp.sum(now["total"], axis=1, keepdims=True), now["part"])
        now = ahead


def attend_kernel(code_ref, len_ref, *rest, sizes, pieces, halves):
    row_refs, rest = rest[: pieces[0]], rest[pieces[0] :]
    k_refs, rest = rest[: pieces[1]], rest[pieces[1] :]
    v_refs, rest = rest[: pieces[2]], rest[pieces[2] :]
    out_refs = rest[:halves]
    acc_ref, m_ref, l_ref, s_ref = rest[halves:]
    batch, heads, head_dim = acc_ref.shape
    count = batch // halves
    m_ref[...] = jnp.full(m_ref.shape, NEG, jnp.float32)
    l_ref[...] = jnp.zeros(l_ref.shape, jnp.float32)
    acc_ref[...] = jnp.zeros(acc_ref.shape, jnp.float32)

    def fold(slot, seq, peak, total, part):
        at = seq
        if halves == 2:
            at = side_of(seq ^ lax.axis_index("seq"), batch) * count + (seq >> 1)
        m_old = m_ref[at]
        m_new = jnp.maximum(m_old, peak)
        a = jnp.exp2(m_old - m_new)
        c = jnp.exp2(peak - m_new)
        m_ref[at] = m_new
        l_ref[at] = l_ref[at] * a + total * c
        acc_ref[at] = acc_ref[at] * a + part * c

    attend_slots((code_ref, len_ref, row_refs, k_refs, v_refs), s_ref, sizes, fold)
    lane = lax.broadcasted_iota(jnp.int32, (heads, TILE), 1)
    stats = jnp.zeros((heads, TILE), jnp.float32)
    for half in range(halves):
        for i in range(count):
            at = half * count + i
            stats = jnp.where(lane == 2 * half * count + i, m_ref[at], stats)
            stats = jnp.where(lane == (2 * half + 1) * count + i, l_ref[at], stats)
            out_refs[half][i * heads : (i + 1) * heads] = acc_ref[at]
    turned = jnp.transpose(stats, (1, 0))
    for half in range(halves):
        out_refs[half][count * heads :, :heads] = turned[2 * half * count : 2 * (half + 1) * count]
        if heads < head_dim:
            out_refs[half][count * heads :, heads:] = jnp.zeros((2 * count, head_dim - heads), jnp.float32)


def side_of(device, n):
    return (device & 1) ^ (device // (n // 2))


def split3(x):
    high = x.astype(jnp.bfloat16).astype(jnp.float32)
    mid = (x - high).astype(jnp.bfloat16).astype(jnp.float32)
    return high, mid, x - high - mid


def pair_kernel(mine_ref, other_ref, out_ref):
    count, rows, head_dim = out_ref.shape
    heads = rows - EXTRA
    base = count * heads
    m1, l1 = mine_ref[base : base + count], mine_ref[base + count :]
    m2, l2 = other_ref[base : base + count], other_ref[base + count :]
    m = jnp.maximum(m1, m2)
    a = jnp.exp2(m1 - m)
    b = jnp.exp2(m2 - m)
    l = a * l1 + b * l2
    some = l > 0.0
    safe = jnp.where(some, l, 1.0)
    inv = jnp.where(some, 1.0 / safe, 0.0)
    lse = jnp.where(some, m + jnp.log2(safe), NEG)
    high, mid, low = split3(lse)
    cols = jnp.transpose(jnp.concatenate([a * inv, b * inv], axis=0), (1, 0))
    line = lax.broadcasted_iota(jnp.int32, (EXTRA, head_dim), 0)
    for i in range(count):
        x = cols[:heads, i : i + 1] * mine_ref[i * heads : (i + 1) * heads]
        y = cols[:heads, count + i : count + i + 1] * other_ref[i * heads : (i + 1) * heads]
        out_ref[i, :heads] = (x + y).astype(jnp.bfloat16)
        pack = jnp.where(line == 0, high[i : i + 1], jnp.where(line == 1, mid[i : i + 1], 0.0))
        out_ref[i, heads:] = jnp.where(line == 2, low[i : i + 1], pack).astype(jnp.bfloat16)


def merge_kernel(in_ref, out_ref):
    n, _, head_dim = in_ref.shape
    heads = out_ref.shape[0]
    lses = []
    for i in range(n):
        tail = in_ref[i, heads:].astype(jnp.float32)
        lses.append(tail[0:1] + tail[1:2] + tail[2:3])
    best = functools.reduce(jnp.maximum, lses)
    ws = [jnp.exp2(x - best) for x in lses]
    inv = 1.0 / functools.reduce(jnp.add, ws)
    eye = lax.broadcasted_iota(jnp.int32, (heads, head_dim), 0) == lax.broadcasted_iota(
        jnp.int32, (heads, head_dim), 1
    )
    acc = jnp.zeros((heads, head_dim), jnp.float32)
    for i in range(n):
        w = jnp.sum(jnp.where(eye, ws[i] * inv, 0.0), axis=1, keepdims=True)
        acc = acc + w * in_ref[i, :heads].astype(jnp.float32)
    out_ref[...] = acc.astype(jnp.bfloat16)


def pack_rows(whole, batch, heads, n, share):
    head_dim = whole.shape[1]
    sums = whole[: batch * heads].reshape(batch, heads, head_dim)
    m = whole[batch * heads : batch * (heads + 1), :heads]
    l = whole[batch * (heads + 1) :, :heads]
    some = l > 0.0
    safe = jnp.where(some, l, 1.0)
    out = jnp.where(some, 1.0 / safe, 0.0)[..., None] * sums
    lse = jnp.where(some, m + jnp.log2(safe), NEG)
    high = lax.reduce_precision(lse, 8, 7)
    mid = lax.reduce_precision(lse - high, 8, 7)
    lines = jnp.stack([x.reshape(n, share) for x in (high, mid, lse - high - mid)], axis=1)
    tail = jnp.zeros((n, EXTRA, head_dim), jnp.float32).at[:, :3, :share].set(lines)
    return jnp.concatenate([out.reshape(n, share, head_dim), tail], axis=1).astype(jnp.bfloat16)


def body(queries, keys, values, lengths, slot_block):
    n = lax.axis_size("seq")
    slots, block, kv, head_dim = keys.shape
    batch = lengths.shape[0]
    share = queries.shape[0]
    heads = share * n // batch
    local = queries.reshape(share, head_dim)
    paired = share == heads and n & (n - 1) == 0 and n > 2
    halves = 2 if paired else 1
    if paired:
        rows = gather_rows(local, n)
        steps = steps_of(n)

        def place(seq):
            away = seq ^ lax.axis_index("seq")
            at = jnp.int32(0)
            for i, step in enumerate(steps):
                hit = (away & step) != 0
                at = at | jnp.where(hit, 1 << i, 0)
                away = away ^ jnp.where(hit, 1, 0)
            return away & 1, at

    else:
        rows = [lax.all_gather(local, "seq", axis=0, tiled=True)]

        def place(seq):
            return jnp.int32(0), seq

    rows = [x.reshape(-1, heads, head_dim) for x in rows]
    parts = kv // 2 if kv % 2 == 0 else 1
    sizes = {"kv": kv, "per_seq": slots * n // batch, "place": place}

    def view_of(cache):
        return pltpu.with_memory_space_constraint(cache.reshape(slots, block, parts, kv // parts, head_dim), pltpu.HBM)

    key_view, value_view = view_of(keys), view_of(values)
    pieces = (2 if slots % 2 == 0 else 1, 1)
    blocks = []
    for view, count in zip((key_view, value_view), pieces):
        for i in range(count):
            blocks.append(spread(view, i * (slots // count), slots // count))
    sums = pl.pallas_call(
        functools.partial(attend_kernel, sizes=sizes, pieces=(len(rows), *pieces), halves=halves),
        in_specs=[SMEM, SMEM] + [VMEM] * (len(rows) + len(blocks)),
        out_specs=[VMEM] * halves,
        out_shape=[pltpu.VMEM((batch // halves * (heads + 2), head_dim), jnp.float32)] * halves,
        scratch_shapes=[pltpu.VMEM((batch, heads, head_dim), jnp.float32)] * 3
        + [pltpu.VMEM((2, heads, block * kv // parts), jnp.float32)],
        compiler_params=limit(24),
        name="attend",
    )(slot_block, lengths, *rows, *blocks)
    if paired:
        other = lax.ppermute(sums[1], "seq", [(i, i ^ 1) for i in range(n)])
        packed = pl.pallas_call(
            pair_kernel,
            out_shape=jax.ShapeDtypeStruct((batch // 2, heads + EXTRA, head_dim), jnp.bfloat16),
            compiler_params=limit(8),
            name="pair",
        )(sums[0], other)
        groups = [[i for i in range(n) if side_of(i, n) == side] for side in range(2)]
    else:
        packed = pack_rows(sums[0], batch, heads, n, share)
        groups = None
    got = lax.all_to_all(packed, "seq", 0, 0, tiled=True, axis_index_groups=groups)
    result = pl.pallas_call(
        merge_kernel,
        out_shape=jax.ShapeDtypeStruct((share, head_dim), jnp.bfloat16),
        compiler_params=limit(8),
        name="merge",
    )(got)
    return result.reshape(share, 1, head_dim)


def solution(mesh):
    placed = (
        P(("grp", "seq"), "head", None),
        P(("grp", "seq"), None, "head", None),
        P(("grp", "seq"), None, "head", None),
        P("grp"),
        P(("grp", "seq")),
    )
    return jax.shard_map(
        body, mesh=mesh, in_specs=placed, out_specs=P(("grp", "seq"), "head", None), check_vma=False
    )
```
